32 devices in a mesh: rows: 2 (over core), cols: 2 (over y), slabs: 2 (over x), site: 4 (over z).
Axes of the slice: x: 2, y: 2, z: 4, core: 2. Of those that a mesh axis runs over, the one named last changes fastest.
Arguments:
- field_values: float32 [768, 16, 16, 128], P(('site', 'rows'), 'cols', 'slabs'), parts along dimension 0, may hold values from 0.5 to 2
- crowding: float32 [768, 16, 16, 128], P(('site', 'rows'), 'cols', 'slabs'), parts along dimension 0, may hold values from 0.5 to 2
Outputs:
- standardized: float32 [768, 16, 16, 128], P(('site', 'rows'), 'cols', 'slabs'), parts along dimension 0
- field_values_end: float32 [768, 16, 16, 128], P(('site', 'rows'), 'cols', 'slabs'), parts along dimension 0
The draws below stay inside these ranges and needn't reach their ends.
There are 4 independent parts, one for each index of `site`. The reference program is written for one: setup_inputs(seed, part) draws one part's arguments, and reference() takes and returns one part's arrays. A program takes and returns all parts, laid end to end along the dimension named above; each array names one. Nothing has to cross between parts.
All inputs are finite; a program needn't handle non-finite values.
Results may differ from the reference program's by a relative error of at most 0.000036.
Values sent between devices are 32-bit elements; how exact they have to be, the bound alone decides.
No kernel may reach another device: no remote copies, remote signals or barrier semaphores. Data moves between devices by JAX's collectives and lax.ppermute only.
A program may use at most 64 MiB of HBM per device.

```python
import jax
import jax.numpy as jnp
from jax import lax

GRID_Y = 192
GRID_X = 16
GRID_Z = 16
LEVELS = 128
STEPS = 6


def levels(own_key, extent, cuts, low, top_value):
    gain, own = 1.0, jax.random.fold_in(own_key, 6)
    for axis_at, shards_of in cuts:
        draws = jnp.exp(jax.random.uniform(jax.random.fold_in(own, axis_at), (shards_of,), jnp.float32, low / len(cuts), top_value / len(cuts)))
        gain = gain * jnp.repeat(draws, extent[axis_at] // shards_of).reshape([-1 if axis == axis_at else 1 for axis in range(len(extent))])
    return gain


def setup_inputs(seed: int = 0, part: int = 0) -> dict:
    keys = jax.random.split(jax.random.key(seed), 3)
    part_splits = jax.random.split(jax.random.fold_in(keys[2], part), 3)
    field_values = jnp.clip(0.5 + 1.5 * jax.random.uniform(part_splits[0], (GRID_Y, GRID_X, GRID_Z, LEVELS), jnp.float32) ** levels(part_splits[0], (GRID_Y, GRID_X, GRID_Z, LEVELS), ((0, 2), (1, 2), (2, 2)), -0.2, 0.2), 0.5, 2.0)
    crowding = jnp.clip(0.5 + 1.5 * jax.random.uniform(part_splits[1], (GRID_Y, GRID_X, GRID_Z, LEVELS), jnp.float32) ** levels(part_splits[1], (GRID_Y, GRID_X, GRID_Z, LEVELS), ((0, 2), (1, 2), (2, 2)), -0.2, 0.2), 0.5, 2.0)
    return {"field_values": field_values, "crowding": crowding}


def inner_cells(values, dims):
    for dim in dims:
        values = lax.slice_in_dim(values, 1, values.shape[dim] - 1, axis=dim)
    return values

def side_cells(values, dim, start, dims):
    others = [other for other in dims if other != dim]
    values = inner_cells(values, others)
    return lax.slice_in_dim(values, start, start + values.shape[dim] - 2, axis=dim)

def advance(padded, crowding):
    middle = inner_cells(padded, (0, 1, 2))
    lower = [side_cells(padded, dim, 0, (0, 1, 2)) for dim in (0, 1, 2)]
    upper = [side_cells(padded, dim, 2, (0, 1, 2)) for dim in (0, 1, 2)]
    spread = lower[0] + upper[0] + lower[1] + upper[1] + lower[2] + upper[2] - 6.0 * middle
    return middle + 0.1 * spread + 0.2 * middle * (1.0 - middle * crowding)

def reference(field_values, crowding):
    for step in range(STEPS):
        field_values = advance(jnp.pad(field_values, ((1, 1), (1, 1), (1, 1), (0, 0)), mode='wrap'), crowding)
    line_mean = lax.optimization_barrier(jnp.mean(field_values, axis=0, keepdims=True))
    centred = field_values - line_mean
    line_variance = lax.optimization_barrier(jnp.mean(centred * centred, axis=0, keepdims=True))
    standardized = centred * lax.rsqrt(line_variance + 0.0001)
    return (standardized, field_values)
```

```python
import functools

import jax
import jax.numpy as jnp
from jax import lax
from jax.experimental import pallas as pl
from jax.experimental.pallas import tpu as pltpu
from jax.sharding import PartitionSpec as P

STEPS = 6
CHUNKS = 2
EPS = 0.0001
VMEM_GRANT = 16 << 20


VMEM_SPEC = pl.BlockSpec(memory_space=pltpu.VMEM)
ANY_SPEC = pl.BlockSpec(memory_space=pl.ANY)


def in_vmem(value):
    return pltpu.with_memory_space_constraint(value, pltpu.VMEM)


def vmem_out(shape):
    return pltpu.VMEM(shape, jnp.float32)


def cost(shape, flops_per_cell, arrays):
    cells = 1
    for size in shape:
        cells *= size
    return pl.CostEstimate(flops=flops_per_cell * cells, bytes_accessed=4 * arrays * cells, transcendentals=0)


def store_faces(row, planes, x_face, z_face):
    last_x, last_z = len(planes) - 1, planes[0].shape[0] - 1
    x_face[0, row] = planes[0]
    x_face[1, row] = planes[last_x]
    for x, plane in enumerate(planes):
        z_face[0, row, x:x + 1, :] = plane[0:1, :]
        z_face[1, row, x:x + 1, :] = plane[last_z:last_z + 1, :]


def open_kernel(start, block, whole, field, x_face, z_face, y_first, y_last, sems):
    rows, xs = field.shape[0], field.shape[1]
    parts = rows // block
    copies = [
        pltpu.make_async_copy(
            whole.at[pl.ds(start + part * block, block)], field.at[pl.ds(part * block, block)], sems.at[part])
        for part in range(parts)
    ]
    for copy in copies:
        copy.start()
    for part, copy in enumerate(copies):
        copy.wait()

        def row_faces(i, carry, part=part):
            row = part * block + i
            store_faces(row, [field[row, x] for x in range(xs)], x_face, z_face)
            return carry

        lax.fori_loop(0, block, row_faces, 0, unroll=2)
    y_first[...] = field[0]
    y_last[...] = field[rows - 1]


def open_chunk(field_values, start, rows):
    _, xs, zs, levels = field_values.shape
    block = rows // 4 if rows % 4 == 0 else rows
    return pl.pallas_call(
        functools.partial(open_kernel, start, block),
        out_shape=(
            vmem_out((rows, xs, zs, levels)),
            vmem_out((2, rows, zs, levels)),
            vmem_out((2, rows, xs, levels)),
            vmem_out((xs, zs, levels)),
            vmem_out((xs, zs, levels)),
        ),
        in_specs=[ANY_SPEC],
        out_specs=(VMEM_SPEC,) * 5,
        scratch_shapes=[pltpu.SemaphoreType.DMA((rows // block,))],
        cost_estimate=cost((rows, xs, zs, levels), 4, 2),
        compiler_params=pltpu.CompilerParams(vmem_limit_bytes=VMEM_GRANT),
        name="open_chunk",
    )(field_values)


def step_kernel(start, last, x_count, z_count, *refs):
    field, crowding, y_before, y_after = refs[:4]
    x_halo = refs[4:4 + x_count]
    z_halo = refs[4 + x_count:4 + x_count + z_count]
    outs = refs[4 + x_count + z_count:]
    if last:
        out, mean_out, square_out = outs
    else:
        out, x_face, z_face, y_first, y_last = outs
    rows, xs, zs, levels = field.shape
    x_before, x_after = (x_halo[0].at[1], x_halo[0].at[0]) if x_count == 1 else x_halo
    z_before, z_after = (z_halo[0].at[1], z_halo[0].at[0]) if z_count == 1 else z_halo
    place = lax.broadcasted_iota(jnp.int32, (zs, levels), 0)
    is_first, is_last = place == 0, place == zs - 1

    def advance(row, below, here, above):
        new = []
        for x in range(xs):
            u = here[x]
            left = x_before[row] if x == 0 else here[x - 1]
            right = x_after[row] if x == xs - 1 else here[x + 1]
            near = jnp.broadcast_to(z_before[row, x:x + 1, :], (zs, levels))
            far = jnp.broadcast_to(z_after[row, x:x + 1, :], (zs, levels))
            near = jnp.where(is_first, near, pltpu.roll(u, 1, 0))
            far = jnp.where(is_last, far, pltpu.roll(u, zs - 1, 0))
            around = (left + right) + (near + far) + (below[x] + above[x])
            new.append(0.1 * around + u * (0.6 - 0.2 * (u * crowding[start + row, x])))
        for x in range(xs):
            out[row, x] = new[x]
        if not last:
            store_faces(row, new, x_face, z_face)
        return new

    def planes(ref, row):
        return [ref[row, x] for x in range(xs)]

    def body(row, total):
        new = advance(row, planes(field, row - 1), planes(field, row), planes(field, row + 1))
        return [a + b for a, b in zip(total, new)] if last else total

    top = [y_before[x] for x in range(xs)]
    new = advance(0, top, planes(field, 0), planes(field, 1))
    total = lax.fori_loop(1, rows - 1, body, new if last else 0, unroll=2)
    bottom = [y_after[x] for x in range(xs)]
    new = advance(rows - 1, planes(field, rows - 2), planes(field, rows - 1), bottom)
    if not last:
        y_first[...] = out[0]
        y_last[...] = out[rows - 1]
        return
    mean = [(a + b) * (1.0 / rows) for a, b in zip(total, new)]

    def squares(row, sums):
        return [s + (out[row, x] - m) * (out[row, x] - m) for x, (s, m) in enumerate(zip(sums, mean))]

    sums = lax.fori_loop(0, rows, squares, [jnp.zeros_like(m) for m in mean], unroll=2)
    for x in range(xs):
        mean_out[x] = mean[x]
        square_out[x] = sums[x]


def step_chunk(field, crowding, y_before, y_after, x_halo, z_halo, start, last):
    rows, xs, zs, levels = field.shape
    if last:
        out_shape = (vmem_out((rows, xs, zs, levels)), vmem_out((xs, zs, levels)), vmem_out((xs, zs, levels)))
    else:
        out_shape = (
            vmem_out((rows, xs, zs, levels)),
            vmem_out((2, rows, zs, levels)),
            vmem_out((2, rows, xs, levels)),
            vmem_out((xs, zs, levels)),
            vmem_out((xs, zs, levels)),
        )
    operands = [field, crowding, y_before, y_after, *x_halo, *z_halo]
    return pl.pallas_call(
        functools.partial(step_kernel, start, last, len(x_halo), len(z_halo)),
        out_shape=out_shape,
        in_specs=[VMEM_SPEC] * len(operands),
        out_specs=(VMEM_SPEC,) * len(out_shape),
        cost_estimate=cost((rows, xs, zs, levels), 16, 3),
        compiler_params=pltpu.CompilerParams(vmem_limit_bytes=VMEM_GRANT),
        name="last_step" if last else "step",
    )(*[in_vmem(operand) for operand in operands])


def close_kernel(block, *refs):
    chunks = (len(refs) - 7) // 1
    fields = refs[:chunks]
    mean_ref, square_ref, scaled, end, stage, sems, end_sems = refs[chunks:]
    xs = fields[0].shape[1]
    rows = fields[0].shape[0]
    copies = []
    for c, field in enumerate(fields):
        copy = pltpu.make_async_copy(field, end.at[pl.ds(c * rows, rows)], end_sems.at[c])
        copy.start()
        copies.append(copy)
    mean = [mean_ref[x] for x in range(xs)]
    gain = [lax.rsqrt(square_ref[x] + EPS) for x in range(xs)]
    piece = 0
    for c, field in enumerate(fields):
        for part in range(rows // block):

            def scale(i, carry, part=part, field=field, c=c):
                row = part * block + i
                for x in range(xs):
                    stage[c * rows + row, x] = (field[row, x] - mean[x]) * gain[x]
                return carry

            lax.fori_loop(0, block, scale, 0, unroll=2)
            at = c * rows + part * block
            copy = pltpu.make_async_copy(
                stage.at[pl.ds(at, block)], scaled.at[pl.ds(at, block)], sems.at[piece])
            copy.start()
            copies.append(copy)
            piece += 1
    for copy in copies:
        copy.wait()


def close(fields, mean, variance):
    rows, xs, zs, levels = fields[0].shape
    whole = (rows * len(fields), xs, zs, levels)
    block = rows // 4 if rows % 4 == 0 else rows
    return pl.pallas_call(
        functools.partial(close_kernel, block),
        out_shape=(jax.ShapeDtypeStruct(whole, jnp.float32),) * 2,
        in_specs=[VMEM_SPEC] * (len(fields) + 2),
        out_specs=(ANY_SPEC,) * 2,
        scratch_shapes=[
            pltpu.VMEM(whole, jnp.float32),
            pltpu.SemaphoreType.DMA((whole[0] // block,)),
            pltpu.SemaphoreType.DMA((len(fields),)),
        ],
        cost_estimate=cost(whole, 3, 4),
        compiler_params=pltpu.CompilerParams(vmem_limit_bytes=VMEM_GRANT),
        name="close",
    )(*[in_vmem(value) for value in (*fields, mean, variance)])


def ring(axis):
    devices = lax.axis_size(axis)
    up = [(i, (i + 1) % devices) for i in range(devices)]
    return devices, up, [(j, i) for i, j in up]


def exchange(face, axis):
    devices, up, down = ring(axis)
    if devices <= 2:
        return (lax.ppermute(face, axis, up),)
    return (lax.ppermute(face[1], axis, up), lax.ppermute(face[0], axis, down))


def local(field_values, crowding):
    length = field_values.shape[0]
    chunks = CHUNKS if length % CHUNKS == 0 else 1
    rows = length // chunks
    _, up, down = ring("rows")
    state = [open_chunk(field_values, c * rows, rows) for c in range(chunks)]
    for step in range(STEPS):
        last = step == STEPS - 1
        halos = [(exchange(s[1], "cols"), exchange(s[2], "slabs")) for s in state]
        before = lax.ppermute(state[-1][4], "rows", up)
        after = lax.ppermute(state[0][3], "rows", down)
        new = []
        for c, (s, (x_halo, z_halo)) in enumerate(zip(state, halos)):
            y_before = before if c == 0 else state[c - 1][4]
            y_after = after if c == chunks - 1 else state[c + 1][3]
            new.append(step_chunk(s[0], crowding, y_before, y_after, x_halo, z_halo, c * rows, last))
        state = new
    means, squares = [s[1] for s in state], [s[2] for s in state]
    packed = jnp.stack([*means, *squares])
    devices = lax.axis_size("rows")
    for hop in range(1, devices):
        other = lax.ppermute(packed, "rows", [(i, (i + hop) % devices) for i in range(devices)])
        means += [other[c] for c in range(chunks)]
        squares += [other[chunks + c] for c in range(chunks)]
    mean = sum(means) * (1.0 / len(means))
    spread = sum(squares) + rows * sum((m - mean) * (m - mean) for m in means)
    variance = spread * (1.0 / (length * devices))
    return close([s[0] for s in state], mean, variance)


def solution(mesh):
    spec = P(("site", "rows"), "cols", "slabs", None)
    return jax.shard_map(local, mesh=mesh, in_specs=(spec, spec), out_specs=(spec, spec), check_vma=False)
```

```python
import functools

import jax
import jax.numpy as jnp
from jax import lax
from jax.experimental import pallas as pl
from jax.experimental.pallas import tpu as pltpu
from jax.sharding import PartitionSpec as P

STEPS = 6
CHUNKS = 3
EPS = 0.0001
VMEM_GRANT = 16 << 20


VMEM_SPEC = pl.BlockSpec(memory_space=pltpu.VMEM)
ANY_SPEC = pl.BlockSpec(memory_space=pl.ANY)
PARAMS = pltpu.CompilerParams(vmem_limit_bytes=VMEM_GRANT)


def in_vmem(value):
    return pltpu.with_memory_space_constraint(value, pltpu.VMEM)


def in_hbm(value):
    return pltpu.with_memory_space_constraint(value, pltpu.HBM)


def vmem_out(*shape):
    return pltpu.VMEM(shape, jnp.float32)


def cost(shape, flops_per_cell, arrays):
    cells = 1
    for size in shape:
        cells *= size
    return pl.CostEstimate(flops=flops_per_cell * cells, bytes_accessed=4 * arrays * cells, transcendentals=0)


def split(length, pieces):
    edges = [length * i // pieces for i in range(pieces + 1)]
    return [(a, b - a) for a, b in zip(edges[:-1], edges[1:]) if b > a]


def store_faces(row, planes, x_face, z_face):
    last_x, last_z = len(planes) - 1, planes[0].shape[0] - 1
    x_face[0, row] = planes[0]
    x_face[1, row] = planes[last_x]
    for x, plane in enumerate(planes):
        z_face[0, row, x:x + 1, :] = plane[0:1, :]
        z_face[1, row, x:x + 1, :] = plane[last_z:last_z + 1, :]


def face_shapes(rows, xs, zs, levels):
    return (
        vmem_out(2, rows, zs, levels),
        vmem_out(2, rows, xs, levels),
        vmem_out(xs, zs, levels),
        vmem_out(xs, zs, levels),
    )


def open_kernel(start, parts, whole, field, x_face, z_face, y_first, y_last, sems):
    rows, xs = field.shape[0], field.shape[1]
    copies = [
        pltpu.make_async_copy(whole.at[pl.ds(start + at, size)], field.at[pl.ds(at, size)], sems.at[part])
        for part, (at, size) in enumerate(parts)
    ]
    for copy in copies:
        copy.start()

    def row_faces(row, carry):
        store_faces(row, [field[row, x] for x in range(xs)], x_face, z_face)
        return carry

    for copy, (at, size) in zip(copies, parts):
        copy.wait()
        lax.fori_loop(at, at + size, row_faces, 0, unroll=2)
    y_first[...] = field[0]
    y_last[...] = field[rows - 1]


def open_chunk(field_values, start, rows):
    _, xs, zs, levels = field_values.shape
    parts = split(rows, 4)
    return pl.pallas_call(
        functools.partial(open_kernel, start, parts),
        out_shape=(vmem_out(rows, xs, zs, levels), *face_shapes(rows, xs, zs, levels)),
        in_specs=[ANY_SPEC],
        out_specs=(VMEM_SPEC,) * 5,
        scratch_shapes=[pltpu.SemaphoreType.DMA((len(parts),))],
        compiler_params=PARAMS,
        cost_estimate=cost((rows, xs, zs, levels), 4, 2),
        name="open_chunk",
    )(in_hbm(field_values))


def update_rows(start, field, crowding, y_before, y_after, x_halo, z_halo, out, finish, total):
    rows, xs, zs, levels = field.shape
    x_before, x_after = (x_halo[0].at[1], x_halo[0].at[0]) if len(x_halo) == 1 else x_halo
    z_before, z_after = (z_halo[0].at[1], z_halo[0].at[0]) if len(z_halo) == 1 else z_halo
    place = lax.broadcasted_iota(jnp.int32, (zs, levels), 0)
    is_first, is_last = place == 0, place == zs - 1

    def planes(ref, row):
        return [ref[row, x] for x in range(xs)]

    def advance(row, below, here, above, total):
        new = []
        for x in range(xs):
            u = here[x]
            left = x_before[row] if x == 0 else here[x - 1]
            right = x_after[row] if x == xs - 1 else here[x + 1]
            near = jnp.broadcast_to(z_before[row, x:x + 1, :], (zs, levels))
            far = jnp.broadcast_to(z_after[row, x:x + 1, :], (zs, levels))
            near = jnp.where(is_first, near, pltpu.roll(u, 1, 0))
            far = jnp.where(is_last, far, pltpu.roll(u, zs - 1, 0))
            around = (left + right) + (near + far) + (below[x] + above[x])
            new.append(0.1 * around + u * (0.6 - 0.2 * (u * crowding[start + row, x])))
        for x in range(xs):
            out[row, x] = new[x]
        return finish(row, new, total)

    def body(row, total):
        return advance(row, planes(field, row - 1), planes(field, row), planes(field, row + 1), total)

    top = [y_before[x] for x in range(xs)]
    bottom = [y_after[x] for x in range(xs)]
    total = advance(0, top, planes(field, 0), planes(field, 1), total)
    total = lax.fori_loop(1, rows - 1, body, total, unroll=2)
    return advance(rows - 1, planes(field, rows - 2), planes(field, rows - 1), bottom, total)


def step_kernel(start, x_count, z_count, *refs):
    field, crowding, y_before, y_after = refs[:4]
    x_halo = refs[4:4 + x_count]
    z_halo = refs[4 + x_count:4 + x_count + z_count]
    out, x_face, z_face, y_first, y_last = refs[4 + x_count + z_count:]

    def finish(row, new, total):
        store_faces(row, new, x_face, z_face)
        return total

    update_rows(start, field, crowding, y_before, y_after, x_halo, z_halo, out, finish, 0)
    y_first[...] = out[0]
    y_last[...] = out[field.shape[0] - 1]


def step_chunk(field, crowding, y_before, y_after, x_halo, z_halo, start):
    rows, xs, zs, levels = field.shape
    operands = [field, crowding, y_before, y_after, *x_halo, *z_halo]
    return pl.pallas_call(
        functools.partial(step_kernel, start, len(x_halo), len(z_halo)),
        out_shape=(vmem_out(rows, xs, zs, levels), *face_shapes(rows, xs, zs, levels)),
        in_specs=[VMEM_SPEC] * len(operands),
        out_specs=(VMEM_SPEC,) * 5,
        compiler_params=PARAMS,
        cost_estimate=cost((rows, xs, zs, levels), 16, 3),
        name="step",
    )(*[in_vmem(operand) for operand in operands])


def merge(groups):
    count, mean, square = groups[0]
    for other_count, other_mean, other_square in groups[1:]:
        both = count + other_count
        apart = other_mean - mean
        mean = mean + apart * (other_count / both)
        square = square + other_square + (apart * apart) * (count * other_count / both)
        count = both
    return count, mean, square


def last_kernel(start, x_count, z_count, earlier, keeps, writes, *refs):
    refs = list(refs)
    field, crowding, y_before, y_after = refs[:4]
    x_halo = refs[4:4 + x_count]
    z_halo = refs[4 + x_count:4 + x_count + z_count]
    rest = refs[4 + x_count + z_count:]
    earlier_stats = rest.pop(0) if earlier else None
    if keeps:
        rest.pop(0)
    out, stats = rest[:2]
    rows, xs = field.shape[0], field.shape[1]

    def finish(row, new, total):
        if total is None:
            return new, [jnp.zeros_like(u) for u in new], [jnp.zeros_like(u) for u in new]
        base, sums, squares = total
        away = [u - b for u, b in zip(new, base)]
        sums = [s + d for s, d in zip(sums, away)]
        squares = [q + d * d for q, d in zip(squares, away)]
        return base, sums, squares

    base, sums, squares = update_rows(
        start, field, crowding, y_before, y_after, x_halo, z_halo, out, finish, None)
    if writes:
        end, sem = rest[2:]
        copy = pltpu.make_async_copy(out, end.at[pl.ds(start, rows)], sem)
        copy.start()
    for x in range(xs):
        mean = base[x] + sums[x] * (1.0 / rows)
        square = squares[x] - sums[x] * sums[x] * (1.0 / rows)
        groups = [(rows, mean, square)]
        if earlier:
            groups = [(earlier, earlier_stats[0, x], earlier_stats[1, x])] + groups
        _, stats[0, x], stats[1, x] = merge(groups)
    if writes:
        copy.wait()


def last_chunk(field, crowding, y_before, y_after, x_halo, z_halo, start, length, earlier_stats, end):
    rows, xs, zs, levels = field.shape
    writes = start + rows < length
    operands = [in_vmem(v) for v in (field, crowding, y_before, y_after, *x_halo, *z_halo)]
    specs = [VMEM_SPEC] * len(operands)
    if earlier_stats is not None:
        operands.append(in_vmem(earlier_stats))
        specs.append(VMEM_SPEC)
    aliases = {}
    keeps = writes and end is not None
    if keeps:
        aliases = {len(operands): 2}
        operands.append(end)
        specs.append(ANY_SPEC)
    outs = [vmem_out(rows, xs, zs, levels), vmem_out(2, xs, zs, levels)]
    out_specs = [VMEM_SPEC] * 2
    if writes:
        outs.append(jax.ShapeDtypeStruct((length, xs, zs, levels), jnp.float32))
        out_specs.append(ANY_SPEC)
    results = pl.pallas_call(
        functools.partial(last_kernel, start, len(x_halo), len(z_halo), start, keeps, writes),
        out_shape=tuple(outs),
        in_specs=specs,
        out_specs=tuple(out_specs),
        input_output_aliases=aliases,
        scratch_shapes=[pltpu.SemaphoreType.DMA] if writes else [],
        compiler_params=PARAMS,
        cost_estimate=cost((rows, xs, zs, levels), 20, 3),
        name="last_step",
    )(*operands)
    return (*results, end) if not writes else results


def close_kernel(chunks, others, parts, has_end, *refs):
    refs = list(refs)
    fields = refs[:chunks]
    stats = refs[chunks:chunks + 1 + others]
    rest = refs[chunks + 1 + others:]
    if has_end:
        rest.pop(0)
    scaled, end, stage, sems, end_sem = rest
    xs = fields[0].shape[1]
    length = stage.shape[0]
    tail = fields[-1].shape[0]
    end_copy = pltpu.make_async_copy(fields[-1], end.at[pl.ds(length - tail, tail)], end_sem)
    end_copy.start()
    means, gains = [], []
    for x in range(xs):
        count, mean, square = merge([(length, s[0, x], s[1, x]) for s in stats])
        means.append(mean)
        gains.append(lax.rsqrt(square * (1.0 / count) + EPS))
    copies = []
    for piece, (c, base, at, size) in enumerate(parts):

        def scale(row, carry, field=fields[c], base=base):
            for x in range(xs):
                stage[base + row, x] = (field[row, x] - means[x]) * gains[x]
            return carry

        lax.fori_loop(at, at + size, scale, 0, unroll=2)
        copy = pltpu.make_async_copy(
            stage.at[pl.ds(base + at, size)], scaled.at[pl.ds(base + at, size)], sems.at[piece])
        copy.start()
        copies.append(copy)
    for copy in copies:
        copy.wait()
    end_copy.wait()


def close(fields, starts, stats, end):
    _, xs, zs, levels = fields[0].shape
    length = sum(f.shape[0] for f in fields)
    whole = (length, xs, zs, levels)
    parts = [
        (c, base, at, size)
        for c, (f, base) in enumerate(zip(fields, starts))
        for at, size in split(f.shape[0], 3)
    ]
    operands = [in_vmem(v) for v in (*fields, *stats)]
    specs = [VMEM_SPEC] * len(operands)
    aliases = {}
    if end is not None:
        aliases = {len(operands): 1}
        operands.append(end)
        specs.append(ANY_SPEC)
    return pl.pallas_call(
        functools.partial(close_kernel, len(fields), len(stats) - 1, parts, end is not None),
        out_shape=(jax.ShapeDtypeStruct(whole, jnp.float32),) * 2,
        in_specs=specs,
        out_specs=(ANY_SPEC,) * 2,
        input_output_aliases=aliases,
        scratch_shapes=[
            pltpu.VMEM(whole, jnp.float32),
            pltpu.SemaphoreType.DMA((len(parts),)),
            pltpu.SemaphoreType.DMA,
        ],
        compiler_params=PARAMS,
        cost_estimate=cost(whole, 3, 4),
        name="close",
    )(*operands)


def ring(axis):
    devices = lax.axis_size(axis)
    up = [(i, (i + 1) % devices) for i in range(devices)]
    return devices, up, [(j, i) for i, j in up]


def exchange(face, axis):
    devices, up, down = ring(axis)
    if devices <= 2:
        return (lax.ppermute(face, axis, up),)
    return (lax.ppermute(face[1], axis, up), lax.ppermute(face[0], axis, down))


def local(field_values, crowding):
    length = field_values.shape[0]
    pieces = split(length, CHUNKS)
    chunks = len(pieces)
    devices, up, down = ring("rows")
    state = [open_chunk(field_values, start, rows) for start, rows in pieces]
    stats = end = None
    for step in range(STEPS):
        last = step == STEPS - 1
        halos = [(exchange(s[1], "cols"), exchange(s[2], "slabs")) for s in state]
        before = lax.ppermute(state[-1][4], "rows", up)
        after = lax.ppermute(state[0][3], "rows", down)
        new = []
        for c, (s, (x_halo, z_halo), (start, _)) in enumerate(zip(state, halos, pieces)):
            y_before = before if c == 0 else state[c - 1][4]
            y_after = after if c == chunks - 1 else state[c + 1][3]
            given = (s[0], crowding, y_before, y_after, x_halo, z_halo, start)
            if last:
                field, stats, end = last_chunk(*given, length, stats, end)
                new.append((field,))
            else:
                new.append(step_chunk(*given))
        state = new
    others = [
        lax.ppermute(stats, "rows", [(i, (i + hop) % devices) for i in range(devices)])
        for hop in range(1, devices)
    ]
    return close([s[0] for s in state], [start for start, _ in pieces], [stats, *others], end)


def solution(mesh):
    spec = P(("site", "rows"), "cols", "slabs", None)
    return jax.shard_map(local, mesh=mesh, in_specs=(spec, spec), out_specs=(spec, spec), check_vma=False)
```

```python
import functools

import jax
import jax.numpy as jnp
from jax import lax
from jax.experimental import pallas as pl
from jax.experimental.pallas import tpu as pltpu
from jax.sharding import PartitionSpec as P

STEPS = 6
CHUNKS = (1, 1, 1)
EPS = 0.0001
VMEM_GRANT = 16 << 20


VMEM_SPEC = pl.BlockSpec(memory_space=pltpu.VMEM)
ANY_SPEC = pl.BlockSpec(memory_space=pl.ANY)
PARAMS = pltpu.CompilerParams(vmem_limit_bytes=VMEM_GRANT)


def in_vmem(value):
    return pltpu.with_memory_space_constraint(value, pltpu.VMEM)


def in_hbm(value):
    return pltpu.with_memory_space_constraint(value, pltpu.HBM)


def vmem_out(*shape):
    return pltpu.VMEM(shape, jnp.float32)


def cost(shape, flops_per_cell, arrays):
    cells = 1
    for size in shape:
        cells *= size
    return pl.CostEstimate(flops=flops_per_cell * cells, bytes_accessed=4 * arrays * cells, transcendentals=0)


def split(length, shares):
    edges = [length * sum(shares[:i]) // sum(shares) for i in range(len(shares) + 1)]
    return [(a, b - a) for a, b in zip(edges[:-1], edges[1:]) if b > a]


def store_faces(row, planes, x_low, x_high, z_faces):
    last_x, last_z = len(planes) - 1, planes[0].shape[0] - 1
    x_low[row] = planes[0]
    x_high[row] = planes[last_x]
    at = 0
    for z_face in z_faces:
        for x in range(z_face.shape[2]):
            z_face[0, row, x:x + 1, :] = planes[at + x][0:1, :]
            z_face[1, row, x:x + 1, :] = planes[at + x][last_z:last_z + 1, :]
        at += z_face.shape[2]


def open_kernel(start, parts, whole, after, field, y_first, y_last, x_face, z_face, sems):
    rows, xs = field.shape[0], field.shape[1]
    copies = [
        pltpu.make_async_copy(whole.at[pl.ds(start + at, size)], field.at[pl.ds(at, size)], sems.at[part])
        for part, (at, size) in enumerate(parts)
    ]
    for copy in copies:
        copy.start()

    def row_faces(row, carry):
        store_faces(row, [field[row, x] for x in range(xs)], x_face.at[0], x_face.at[1], [z_face])
        return carry

    for copy, (at, size) in zip(copies, parts):
        copy.wait()
        lax.fori_loop(at, at + size, row_faces, 0, unroll=4)
    y_first[...] = field[0]
    y_last[...] = field[rows - 1]


def open_chunk(field_values, after, start, rows):
    _, xs, zs, levels = field_values.shape
    parts = split(rows, (1,) * 4)
    outs = [vmem_out(rows, xs, zs, levels), vmem_out(xs, zs, levels), vmem_out(xs, zs, levels)]
    outs += [vmem_out(2, rows, zs, levels), vmem_out(2, rows, xs, levels)]
    return pl.pallas_call(
        functools.partial(open_kernel, start, parts),
        out_shape=tuple(outs),
        in_specs=[ANY_SPEC] * 2,
        out_specs=(VMEM_SPEC,) * len(outs),
        scratch_shapes=[pltpu.SemaphoreType.DMA((len(parts),))],
        compiler_params=PARAMS,
        cost_estimate=cost((rows, xs, zs, levels), 4, 2),
        name="open_chunk",
    )(in_hbm(field_values), after)


def update_rows(start, span, field, crowding, y_before, y_after, x_before, x_after, z_before, z_after,
                out, finish, total):
    rows, xs, zs, levels = field.shape
    x0, x1 = span
    place = lax.broadcasted_iota(jnp.int32, (zs, levels), 0)
    is_first, is_last = place == 0, place == zs - 1

    def planes(ref, row):
        return [ref[row, x] for x in range(x0, x1)]

    def advance(row, below, here, above, total):
        first = x_before[row] if x0 == 0 else field[row, x0 - 1]
        final = x_after[row] if x1 == xs else field[row, x1]
        along = [first, *here, final]
        new = []
        for i, u in enumerate(here):
            near = jnp.broadcast_to(z_before[row, i:i + 1, :], (zs, levels))
            far = jnp.broadcast_to(z_after[row, i:i + 1, :], (zs, levels))
            near = jnp.where(is_first, near, pltpu.roll(u, 1, 0))
            far = jnp.where(is_last, far, pltpu.roll(u, zs - 1, 0))
            around = (along[i] + along[i + 2]) + (near + far) + (below[i] + above[i])
            new.append(0.1 * around + u * (0.6 - 0.2 * (u * crowding[start + row, x0 + i])))
        for i, u in enumerate(new):
            out[row, i] = u
        return finish(row, new, total)

    def body(row, total):
        return advance(row, planes(field, row - 1), planes(field, row), planes(field, row + 1), total)

    top = [y_before[x] for x in range(x0, x1)]
    bottom = [y_after[x] for x in range(x0, x1)]
    total = advance(0, top, planes(field, 0), planes(field, 1), total)
    total = lax.fori_loop(1, rows - 1, body, total, unroll=3 * xs // (x1 - x0))
    return advance(rows - 1, planes(field, rows - 2), planes(field, rows - 1), bottom, total)


def sides(halo):
    return (halo[0].at[1], halo[0].at[0]) if len(halo) == 1 else tuple(halo)


def step_kernel(start, x_count, z_count, halves, *refs):
    field, crowding, y_before, y_after = refs[:4]
    x_before, x_after = sides(refs[4:4 + x_count])
    z_before, z_after = sides(refs[4 + x_count:4 + x_count + z_count])
    outs = refs[5 + x_count + z_count:]
    out, y_first, y_last = outs[:3]
    if halves:
        x_low, x_high, *z_faces = outs[3:]
    else:
        x_face, *z_faces = outs[3:]
        x_low, x_high = x_face.at[0], x_face.at[1]

    def finish(row, new, total):
        store_faces(row, new, x_low, x_high, z_faces)
        return total

    update_rows(start, (0, field.shape[1]), field, crowding, y_before, y_after, x_before, x_after,
                z_before, z_after, out, finish, 0)
    y_first[...] = out[0]
    y_last[...] = out[field.shape[0] - 1]


def step_chunk(field, crowding, y_before, y_after, x_halo, z_halo, start, after, halves):
    rows, xs, zs, levels = field.shape
    operands = [field, crowding, y_before, y_after, *x_halo, *z_halo, after]
    outs = [vmem_out(rows, xs, zs, levels), vmem_out(xs, zs, levels), vmem_out(xs, zs, levels)]
    if halves:
        cut = half(xs)
        outs += [vmem_out(rows, zs, levels)] * 2
        outs += [vmem_out(2, rows, cut, levels), vmem_out(2, rows, xs - cut, levels)]
    else:
        outs += [vmem_out(2, rows, zs, levels), vmem_out(2, rows, xs, levels)]
    return pl.pallas_call(
        functools.partial(step_kernel, start, len(x_halo), len(z_halo), halves),
        out_shape=tuple(outs),
        in_specs=[VMEM_SPEC] * len(operands),
        out_specs=(VMEM_SPEC,) * len(outs),
        compiler_params=PARAMS,
        cost_estimate=cost((rows, xs, zs, levels), 16, 3),
        name="step",
    )(*[in_vmem(operand) for operand in operands])


def half(xs):
    return xs // 2


def merge(groups):
    count, mean, square = groups[0]
    for other_count, other_mean, other_square in groups[1:]:
        both = count + other_count
        apart = other_mean - mean
        mean = mean + apart * (other_count / both)
        square = square + other_square + (apart * apart) * (count * other_count / both)
        count = both
    return count, mean, square


def last_kernel(start, span, length, x_count, z_count, earlier, keeps, writes, waits, *refs):
    refs = list(refs)
    xs = refs[0].shape[1]
    x0, x1 = span
    field, crowding, y_before, y_after = refs[:4]
    x_halo = refs[4:4 + x_count]
    z_before, z_after = sides(refs[4 + x_count:4 + x_count + z_count])
    rest = refs[4 + x_count + z_count:]
    if x0 == 0 and x1 == xs:
        x_before, x_after = sides(x_halo)
    else:
        x_before = x_after = x_halo[0]
    earlier_stats = rest.pop(0) if earlier else None
    rest = rest[keeps + waits:]
    out, stats = rest[:2]
    rows = field.shape[0]

    def finish(row, new, total):
        if total is None:
            return new, [jnp.zeros_like(u) for u in new], [jnp.zeros_like(u) for u in new]
        base, sums, squares = total
        away = [u - b for u, b in zip(new, base)]
        sums = [s + d for s, d in zip(sums, away)]
        squares = [q + d * d for q, d in zip(squares, away)]
        return base, sums, squares

    base, sums, squares = update_rows(
        start, span, field, crowding, y_before, y_after, x_before, x_after, z_before, z_after,
        out, finish, None)
    if writes:
        end, sem = rest[2:]
        copy = pltpu.make_async_copy(out, end.at[pl.ds(start, rows), pl.ds(x0, x1 - x0)], sem)
        copy.start()
    for i in range(x1 - x0):
        mean = base[i] + sums[i] * (1.0 / rows)
        square = squares[i] - sums[i] * sums[i] * (1.0 / rows)
        groups = [(rows, mean, square)]
        if earlier:
            groups = [(start, earlier_stats[0, x0 + i], earlier_stats[1, x0 + i])] + groups
        _, stats[0, i], stats[1, i] = merge(groups)
    if writes:
        copy.wait()


def last_chunk(field, crowding, y_before, y_after, x_halo, z_halo, start, length, span, earlier_stats, end,
               writes, wait=None):
    rows, xs, zs, levels = field.shape
    wide = span[1] - span[0]
    operands = [in_vmem(v) for v in (field, crowding, y_before, y_after, *x_halo, *z_halo)]
    specs = [VMEM_SPEC] * len(operands)
    if earlier_stats is not None:
        operands.append(in_vmem(earlier_stats))
        specs.append(VMEM_SPEC)
    aliases = {}
    keeps = writes and end is not None
    if keeps:
        aliases = {len(operands): 2}
        operands.append(end)
        specs.append(ANY_SPEC)
    if wait is not None:
        operands.append(in_hbm(wait))
        specs.append(ANY_SPEC)
    outs = [vmem_out(rows, wide, zs, levels), vmem_out(2, wide, zs, levels)]
    out_specs = [VMEM_SPEC] * 2
    if writes:
        outs.append(jax.ShapeDtypeStruct((length, xs, zs, levels), jnp.float32))
        out_specs.append(ANY_SPEC)
    return pl.pallas_call(
        functools.partial(
            last_kernel, start, span, length, len(x_halo), len(z_halo), earlier_stats is not None, keeps, writes,
            wait is not None),
        out_shape=tuple(outs),
        in_specs=specs,
        out_specs=tuple(out_specs),
        input_output_aliases=aliases,
        scratch_shapes=[pltpu.SemaphoreType.DMA] if writes else [],
        compiler_params=PARAMS,
        cost_estimate=cost((rows, wide, zs, levels), 20, 3),
        name="last_step",
    )(*operands)


def write_kernel(start, span, field, end_in, end, sem):
    copy = pltpu.make_async_copy(
        field, end.at[pl.ds(start, field.shape[0]), pl.ds(span[0], field.shape[1])], sem)
    copy.start()
    copy.wait()


def write_part(field, start, span, end):
    return pl.pallas_call(
        functools.partial(write_kernel, start, span),
        out_shape=jax.ShapeDtypeStruct(end.shape, end.dtype),
        in_specs=[VMEM_SPEC, ANY_SPEC],
        out_specs=ANY_SPEC,
        input_output_aliases={1: 0},
        scratch_shapes=[pltpu.SemaphoreType.DMA],
        compiler_params=PARAMS,
        cost_estimate=cost(field.shape, 4, 2),
        name="write_part",
    )(in_vmem(field), end)


def close_kernel(starts, span, others, parts, keeps, left_span, *refs):
    refs = list(refs)
    chunks = len(starts)
    fields = refs[:chunks]
    stats = refs[chunks:chunks + 1 + others]
    rest = refs[chunks + 1 + others:]
    copies = []
    if left_span:
        left, rest = rest[0], rest[1 + keeps:]
        scaled, end, stage, sems, end_sem = rest
        copies.append(pltpu.make_async_copy(
            left, end.at[pl.ds(starts[-1], left.shape[0]), pl.ds(left_span[0], left.shape[1])], end_sem))
        copies[0].start()
    else:
        scaled, stage, sems = rest[keeps:]
    x0, x1 = span
    wide = x1 - x0
    length = stage.shape[0]
    means, gains = [], []
    for i in range(wide):
        count, mean, square = merge([(length, s[0, i], s[1, i]) for s in stats])
        means.append(mean)
        gains.append(lax.rsqrt(square * (1.0 / count) + EPS))
    for piece, (c, at, size) in enumerate(parts):
        base, shift = starts[c], 0 if c == chunks - 1 else x0

        def scale(row, carry, field=fields[c], base=base, shift=shift):
            for i in range(wide):
                stage[base + row, i] = (field[row, shift + i] - means[i]) * gains[i]
            return carry

        lax.fori_loop(at, at + size, scale, 0, unroll=8)
        copy = pltpu.make_async_copy(
            stage.at[pl.ds(base + at, size)], scaled.at[pl.ds(base + at, size), pl.ds(x0, wide)], sems.at[piece])
        copy.start()
        copies.append(copy)
    for copy in copies:
        copy.wait()


def close(fields, starts, span, stats, scaled, end, left, left_span):
    _, xs, zs, levels = fields[0].shape
    length = sum(f.shape[0] for f in fields)
    wide = span[1] - span[0]
    whole = jax.ShapeDtypeStruct((length, xs, zs, levels), jnp.float32)
    parts = [(c, at, size) for c, f in enumerate(fields) for at, size in split(f.shape[0], (1,) * 2)]
    operands = [in_vmem(v) for v in (*fields, *stats)] + ([in_vmem(left)] if left_span else [])
    specs = [VMEM_SPEC] * len(operands)
    aliases = {}
    for place, kept in enumerate((scaled, end) if left_span else (scaled,)):
        if kept is not None:
            aliases[len(operands)] = place
            operands.append(kept)
            specs.append(ANY_SPEC)
    outs = (whole, whole) if left_span else (whole,)
    scratch = [pltpu.VMEM((length, wide, zs, levels), jnp.float32), pltpu.SemaphoreType.DMA((len(parts),))]
    results = pl.pallas_call(
        functools.partial(close_kernel, starts, span, len(stats) - 1, parts, len(aliases), left_span),
        out_shape=outs,
        in_specs=specs,
        out_specs=(ANY_SPEC,) * len(outs),
        input_output_aliases=aliases,
        scratch_shapes=scratch + ([pltpu.SemaphoreType.DMA] if left_span else []),
        compiler_params=PARAMS,
        cost_estimate=cost((length, wide, zs, levels), 3, 4),
        name="close",
    )(*operands)
    return results if left_span else (results[0], end)


def ring(axis):
    devices = lax.axis_size(axis)
    up = [(i, (i + 1) % devices) for i in range(devices)]
    return devices, up, [(j, i) for i, j in up]


def exchange(face, axis):
    devices, up, down = ring(axis)
    if devices <= 2:
        return (lax.ppermute(face, axis, up),)
    return (lax.ppermute(face[1], axis, up), lax.ppermute(face[0], axis, down))


def local(field_values, crowding):
    length, xs = field_values.shape[:2]
    pieces = split(length, CHUNKS)
    starts = [start for start, _ in pieces]
    chunks = len(pieces)
    devices, up, down = ring("rows")
    _, x_up, x_down = ring("cols")
    state = []
    for start, rows in pieces:
        state.append(open_chunk(field_values, state[-1][1] if state else field_values, start, rows))
    for step in range(STEPS - 1):
        halos = [(exchange(s[3], "cols"), exchange(s[4], "slabs")) for s in state]
        before = lax.ppermute(state[-1][2], "rows", up)
        after = lax.ppermute(state[0][1], "rows", down)
        new = []
        for c, (s, (x_halo, z_halo), start) in enumerate(zip(state, halos, starts)):
            y_before = before if c == 0 else state[c - 1][2]
            y_after = after if c == chunks - 1 else state[c + 1][1]
            halves = step == STEPS - 2 and c == chunks - 1
            new.append(step_chunk(s[0], crowding, y_before, y_after, x_halo, z_halo, start,
                                  new[-1][1] if new else s[1], halves))
        state = new
    before = lax.ppermute(state[-1][2], "rows", up)
    after = lax.ppermute(state[0][1], "rows", down)
    fields, stats, end = [], None, None
    for c, s in enumerate(state[:-1]):
        y_before = before if c == 0 else state[c - 1][2]
        field, stats, end = last_chunk(
            s[0], crowding, y_before, state[c + 1][1], exchange(s[3], "cols"), exchange(s[4], "slabs"),
            starts[c], length, (0, xs), stats, end, True)
        fields.append(field)
    field, _, _, x_low, x_high, *z_faces = state[-1]
    y_before = before if chunks == 1 else state[-2][2]
    cut = half(xs)
    hops = [[(i, (i + hop) % devices) for i in range(devices)] for hop in range(1, devices)]

    def finish_half(span, x_halo, z_face, wait):
        part, sums = last_chunk(field, crowding, y_before, after, (x_halo,), exchange(z_face, "slabs"),
                                starts[-1], length, span, stats, None, False, wait)
        return part, [sums, *[lax.ppermute(sums, "rows", hop) for hop in hops]]

    low_span, high_span = (0, cut), (cut, xs)
    low, low_sums = finish_half(low_span, lax.ppermute(x_high, "cols", x_up), z_faces[0], None)
    end = write_part(low, starts[-1], low_span, end)
    high, high_sums = finish_half(high_span, lax.ppermute(x_low, "cols", x_down), z_faces[1], end)
    scaled, end = close((*fields, low), starts, low_span, low_sums, None, end, high, high_span)
    return close((*fields, high), starts, high_span, high_sums, scaled, end, None, None)


def solution(mesh):
    spec = P(("site", "rows"), "cols", "slabs", None)
    return jax.shard_map(local, mesh=mesh, in_specs=(spec, spec), out_specs=(spec, spec), check_vma=False)
```

```python
import functools

import jax
import jax.numpy as jnp
from jax import lax
from jax.experimental import pallas as pl
from jax.experimental.pallas import tpu as pltpu
from jax.sharding import PartitionSpec as P


STEPS = 6
CHUNKS = (1, 1, 1)
EPS = 0.0001
VMEM_GRANT = 16 << 20


VMEM_SPEC = pl.BlockSpec(memory_space=pltpu.VMEM)
ANY_SPEC = pl.BlockSpec(memory_space=pl.ANY)
PARAMS = pltpu.CompilerParams(vmem_limit_bytes=VMEM_GRANT)


def in_vmem(value):
    return pltpu.with_memory_space_constraint(value, pltpu.VMEM)


def in_hbm(value):
    return pltpu.with_memory_space_constraint(value, pltpu.HBM)


def vmem_out(*shape):
    return pltpu.VMEM(shape, jnp.float32)


def cost(shape, flops_per_cell, arrays):
    cells = 1
    for size in shape:
        cells *= size
    return pl.CostEstimate(flops=flops_per_cell * cells, bytes_accessed=4 * arrays * cells, transcendentals=0)


def split(length, shares):
    edges = [length * sum(shares[:i]) // sum(shares) for i in range(len(shares) + 1)]
    return [(a, b - a) for a, b in zip(edges[:-1], edges[1:]) if b > a]


def store_faces(row, planes, x_low, x_high, z_faces):
    last_x, last_z = len(planes) - 1, planes[0].shape[0] - 1
    x_low[row] = planes[0]
    x_high[row] = planes[last_x]
    at = 0
    for z_face in z_faces:
        for x in range(z_face.shape[2]):
            z_face[0, row, x:x + 1, :] = planes[at + x][0:1, :]
            z_face[1, row, x:x + 1, :] = planes[at + x][last_z:last_z + 1, :]
        at += z_face.shape[2]


def open_kernel(start, parts, whole, after, field, y_first, y_last, x_face, z_face, sems):
    rows, xs = field.shape[0], field.shape[1]
    copies = [
        pltpu.make_async_copy(whole.at[pl.ds(start + at, size)], field.at[pl.ds(at, size)], sems.at[part])
        for part, (at, size) in enumerate(parts)
    ]
    for copy in copies:
        copy.start()

    def row_faces(row, carry):
        store_faces(row, [field[row, x] for x in range(xs)], x_face.at[0], x_face.at[1], [z_face])
        return carry

    for copy, (at, size) in zip(copies, parts):
        copy.wait()
        lax.fori_loop(at, at + size, row_faces, 0, unroll=4)
    y_first[...] = field[0]
    y_last[...] = field[rows - 1]


def open_chunk(field_values, after, start, rows):
    _, xs, zs, levels = field_values.shape
    parts = split(rows, (1,) * 4)
    outs = [vmem_out(rows, xs, zs, levels), vmem_out(xs, zs, levels), vmem_out(xs, zs, levels)]
    outs += [vmem_out(2, rows, zs, levels), vmem_out(2, rows, xs, levels)]
    return pl.pallas_call(
        functools.partial(open_kernel, start, parts),
        out_shape=tuple(outs),
        in_specs=[ANY_SPEC] * 2,
        out_specs=(VMEM_SPEC,) * len(outs),
        scratch_shapes=[pltpu.SemaphoreType.DMA((len(parts),))],
        compiler_params=PARAMS,
        cost_estimate=cost((rows, xs, zs, levels), 4, 2),
        name="open_chunk",
    )(in_hbm(field_values), after)


def update_rows(start, span, field, crowding, y_before, y_after, x_before, x_after, z_before, z_after,
                out, finish, total):
    rows, xs, zs, levels = field.shape
    x0, x1 = span
    place = lax.broadcasted_iota(jnp.int32, (zs, levels), 0)
    is_first, is_last = place == 0, place == zs - 1

    def planes(ref, row):
        return [ref[row, x] for x in range(x0, x1)]

    def advance(row, below, here, above, total):
        first = x_before[row] if x0 == 0 else field[row, x0 - 1]
        final = x_after[row] if x1 == xs else field[row, x1]
        along = [first, *here, final]
        new = []
        for i, u in enumerate(here):
            near = jnp.broadcast_to(z_before[row, i:i + 1, :], (zs, levels))
            far = jnp.broadcast_to(z_after[row, i:i + 1, :], (zs, levels))
            near = jnp.where(is_first, near, pltpu.roll(u, 1, 0))
            far = jnp.where(is_last, far, pltpu.roll(u, zs - 1, 0))
            around = (along[i] + along[i + 2]) + (near + far) + (below[i] + above[i])
            new.append(0.1 * around + u * (0.6 - 0.2 * (u * crowding[start + row, x0 + i])))
        for i, u in enumerate(new):
            out[row, i] = u
        return finish(row, new, total)

    def body(row, total):
        return advance(row, planes(field, row - 1), planes(field, row), planes(field, row + 1), total)

    top = [y_before[x] for x in range(x0, x1)]
    bottom = [y_after[x] for x in range(x0, x1)]
    total = advance(0, top, planes(field, 0), planes(field, 1), total)
    total = lax.fori_loop(1, rows - 1, body, total, unroll=3 * xs // (x1 - x0))
    return advance(rows - 1, planes(field, rows - 2), planes(field, rows - 1), bottom, total)


def sides(halo):
    return (halo[0].at[1], halo[0].at[0]) if len(halo) == 1 else tuple(halo)


def step_kernel(start, x_count, z_count, halves, gathers, *refs):
    field, crowding, y_before, y_after = refs[:4]
    x_before, x_after = sides(refs[4:4 + x_count])
    z_before, z_after = sides(refs[4 + x_count:4 + x_count + z_count])
    held = refs[5 + x_count + z_count:5 + x_count + z_count + 2 * gathers]
    outs = refs[5 + x_count + z_count + 2 * gathers:]
    out, y_first, y_last = outs[:3]
    if halves:
        x_low, x_high, *z_faces = outs[3:7]
    else:
        x_face, *z_faces = outs[3:]
        x_low, x_high = x_face.at[0], x_face.at[1]

    def finish(row, new, total):
        store_faces(row, new, x_low, x_high, z_faces)
        return total

    update_rows(start, (0, field.shape[1]), field, crowding, y_before, y_after, x_before, x_after,
                z_before, z_after, out, finish, 0)
    y_first[...] = out[0]
    y_last[...] = out[field.shape[0] - 1]
    if gathers:
        x_all, z_all = outs[7:]
        at = 0
        for low, face in zip(held[:gathers], held[gathers:]):
            rows = low.shape[0]
            x_all[at:at + rows] = low[...]
            z_all[:, at:at + rows] = face[...]
            at += rows


def step_chunk(field, crowding, y_before, y_after, x_halo, z_halo, start, after, halves, held):
    rows, xs, zs, levels = field.shape
    gathers = len(held)
    operands = [field, crowding, y_before, y_after, *x_halo, *z_halo, after]
    operands += [low for low, _ in held] + [face for _, face in held]
    outs = [vmem_out(rows, xs, zs, levels), vmem_out(xs, zs, levels), vmem_out(xs, zs, levels)]
    if halves:
        cut = half(xs)
        outs += [vmem_out(rows, zs, levels)] * 2
        outs += [vmem_out(2, rows, cut, levels), vmem_out(2, rows, xs - cut, levels)]
        if gathers:
            outs += [vmem_out(start, zs, levels), vmem_out(2, start, xs - cut, levels)]
    else:
        outs += [vmem_out(2, rows, zs, levels), vmem_out(2, rows, xs, levels)]
    return pl.pallas_call(
        functools.partial(step_kernel, start, len(x_halo), len(z_halo), halves, gathers),
        out_shape=tuple(outs),
        in_specs=[VMEM_SPEC] * len(operands),
        out_specs=(VMEM_SPEC,) * len(outs),
        compiler_params=PARAMS,
        cost_estimate=cost((rows, xs, zs, levels), 16, 3),
        name="step",
    )(*[in_vmem(operand) for operand in operands])


def half(xs):
    return xs // 2


def merge(groups):
    count, mean, square = groups[0]
    for other_count, other_mean, other_square in groups[1:]:
        both = count + other_count
        apart = other_mean - mean
        mean = mean + apart * (other_count / both)
        square = square + other_square + (apart * apart) * (count * other_count / both)
        count = both
    return count, mean, square


def last_kernel(start, span, halo_at, z_count, earlier, waits, *refs):
    field, crowding, y_before, y_after, x_halo = refs[:5]
    x0, x1 = span
    rows = field.shape[0]
    here = pl.ds(halo_at, rows)
    x_side = x_halo.at[here]
    z_before, z_after = [side.at[here] for side in sides(refs[5:5 + z_count])]
    rest = refs[5 + z_count:]
    earlier_stats = rest[0] if earlier else None
    out, stats = rest[earlier + waits:]

    def finish(row, new, total):
        if total is None:
            return new, [jnp.zeros_like(u) for u in new], [jnp.zeros_like(u) for u in new]
        base, sums, squares = total
        away = [u - b for u, b in zip(new, base)]
        sums = [s + d for s, d in zip(sums, away)]
        squares = [q + d * d for q, d in zip(squares, away)]
        return base, sums, squares

    base, sums, squares = update_rows(
        start, span, field, crowding, y_before, y_after, x_side, x_side, z_before, z_after,
        out, finish, None)
    for i in range(x1 - x0):
        mean = base[i] + sums[i] * (1.0 / rows)
        square = squares[i] - sums[i] * sums[i] * (1.0 / rows)
        groups = [(rows, mean, square)]
        if earlier:
            groups = [(start, earlier_stats[0, i], earlier_stats[1, i])] + groups
        _, stats[0, i], stats[1, i] = merge(groups)


def last_chunk(field, crowding, y_before, y_after, x_halo, z_halo, start, span, halo_at, earlier_stats, wait):
    rows, _, zs, levels = field.shape
    wide = span[1] - span[0]
    operands = [in_vmem(v) for v in (field, crowding, y_before, y_after, x_halo, *z_halo)]
    specs = [VMEM_SPEC] * len(operands)
    if earlier_stats is not None:
        operands.append(in_vmem(earlier_stats))
        specs.append(VMEM_SPEC)
    if wait is not None:
        operands.append(in_hbm(wait))
        specs.append(ANY_SPEC)
    return pl.pallas_call(
        functools.partial(
            last_kernel, start, span, halo_at, len(z_halo), earlier_stats is not None, wait is not None),
        out_shape=(vmem_out(rows, wide, zs, levels), vmem_out(2, wide, zs, levels)),
        in_specs=specs,
        out_specs=(VMEM_SPEC,) * 2,
        compiler_params=PARAMS,
        cost_estimate=cost((rows, wide, zs, levels), 20, 3),
        name="last_step",
    )(*operands)


def part_copies(parts, starts, span, end, sems):
    return [
        pltpu.make_async_copy(
            part, end.at[pl.ds(start, part.shape[0]), pl.ds(span[0], part.shape[1])], sems.at[c])
        for c, (part, start) in enumerate(zip(parts, starts))
    ]


def write_kernel(starts, span, *refs):
    chunks = len(starts)
    end, sems = refs[-2:]
    copies = part_copies(refs[:chunks], starts, span, end, sems)
    for copy in copies:
        copy.start()
    for copy in copies:
        copy.wait()


def write_parts(parts, starts, span, end):
    return pl.pallas_call(
        functools.partial(write_kernel, starts, span),
        out_shape=jax.ShapeDtypeStruct(end.shape, end.dtype),
        in_specs=[VMEM_SPEC] * len(parts) + [ANY_SPEC],
        out_specs=ANY_SPEC,
        input_output_aliases={len(parts): 0},
        scratch_shapes=[pltpu.SemaphoreType.DMA((len(parts),))],
        compiler_params=PARAMS,
        cost_estimate=cost(parts[0].shape, 4 * len(parts), 2),
        name="write_parts",
    )(*[in_vmem(part) for part in parts], end)


def close_kernel(starts, span, others, pieces, first, *refs):
    chunks = len(starts)
    parts = refs[:chunks]
    stats = refs[chunks:chunks + 1 + others]
    copies = []
    if first:
        scaled, end, stage, sems, end_sems = refs[chunks + 1 + others:]
        copies = part_copies(parts, starts, span, end, end_sems)
        for copy in copies:
            copy.start()
    else:
        scaled, stage, sems = refs[chunks + 2 + others:]
    x0, x1 = span
    wide = x1 - x0
    length = stage.shape[0]
    means, gains = [], []
    for i in range(wide):
        count, mean, square = merge([(length, s[0, i], s[1, i]) for s in stats])
        means.append(mean)
        gains.append(lax.rsqrt(square * (1.0 / count) + EPS))
    for piece, (c, at, size) in enumerate(pieces):
        base = starts[c]

        def scale(row, carry, part=parts[c], base=base):
            for i in range(wide):
                stage[base + row, i] = (part[row, i] - means[i]) * gains[i]
            return carry

        lax.fori_loop(at, at + size, scale, 0, unroll=8)
        copy = pltpu.make_async_copy(
            stage.at[pl.ds(base + at, size)], scaled.at[pl.ds(base + at, size), pl.ds(x0, wide)], sems.at[piece])
        copy.start()
        copies.append(copy)
    for copy in copies:
        copy.wait()


def close(parts, starts, span, stats, shape, scaled):
    first = scaled is None
    length, _, zs, levels = shape
    wide = span[1] - span[0]
    whole = jax.ShapeDtypeStruct(shape, jnp.float32)
    pieces = [(c, at, size) for c, f in enumerate(parts) for at, size in split(f.shape[0], (1,) * 2)]
    operands = [in_vmem(v) for v in (*parts, *stats)]
    specs = [VMEM_SPEC] * len(operands)
    if not first:
        operands.append(scaled)
        specs.append(ANY_SPEC)
    outs = (whole, whole) if first else (whole,)
    scratch = [pltpu.VMEM((length, wide, zs, levels), jnp.float32), pltpu.SemaphoreType.DMA((len(pieces),))]
    return pl.pallas_call(
        functools.partial(close_kernel, starts, span, len(stats) - 1, pieces, first),
        out_shape=outs,
        in_specs=specs,
        out_specs=(ANY_SPEC,) * len(outs),
        input_output_aliases={} if first else {len(operands) - 1: 0},
        scratch_shapes=scratch + ([pltpu.SemaphoreType.DMA((len(parts),))] if first else []),
        compiler_params=PARAMS,
        cost_estimate=cost((length, wide, zs, levels), 3, 4),
        name="close",
    )(*operands)


def ring(axis):
    devices = lax.axis_size(axis)
    up = [(i, (i + 1) % devices) for i in range(devices)]
    return devices, up, [(j, i) for i, j in up]


def exchange(face, axis):
    devices, up, down = ring(axis)
    if devices <= 2:
        return (lax.ppermute(face, axis, up),)
    return (lax.ppermute(face[1], axis, up), lax.ppermute(face[0], axis, down))


def local(field_values, crowding):
    length, xs = field_values.shape[:2]
    pieces = split(length, CHUNKS)
    starts = [start for start, _ in pieces]
    chunks = len(pieces)
    devices, up, down = ring("rows")
    _, x_up, x_down = ring("cols")
    state = []
    for start, rows in pieces:
        state.append(open_chunk(field_values, state[-1][1] if state else field_values, start, rows))
    for step in range(STEPS - 1):
        halos = [(exchange(s[3], "cols"), exchange(s[4], "slabs")) for s in state]
        before = lax.ppermute(state[-1][2], "rows", up)
        after = lax.ppermute(state[0][1], "rows", down)
        new = []
        for c, (s, (x_halo, z_halo), start) in enumerate(zip(state, halos, starts)):
            y_before = before if c == 0 else state[c - 1][2]
            y_after = after if c == chunks - 1 else state[c + 1][1]
            halves = step == STEPS - 2
            held = [(n[3], n[6]) for n in new] if halves and c == chunks - 1 else []
            new.append(step_chunk(s[0], crowding, y_before, y_after, x_halo, z_halo, start,
                                  new[-1][1] if new else s[1], halves, held))
        state = new
    before = lax.ppermute(state[-1][2], "rows", up)
    after = lax.ppermute(state[0][1], "rows", down)
    hops = [[(i, (i + hop) % devices) for i in range(devices)] for hop in range(1, devices)]
    cut = half(xs)
    low_span, high_span = (0, cut), (cut, xs)

    def last_half(span, x_halos, z_halos, offsets, wait):
        parts, stats = [], None
        for c, s in enumerate(state):
            y_before = before if c == 0 else state[c - 1][2]
            y_after = after if c == chunks - 1 else state[c + 1][1]
            part, stats = last_chunk(
                s[0], crowding, y_before, y_after, x_halos[c], z_halos[c], starts[c], span, offsets[c], stats,
                wait if c == chunks - 1 else None)
            parts.append(part)
        return parts, [stats, *[lax.ppermute(stats, "rows", hop) for hop in hops]]

    def send(x_face, pairs, z_face):
        x_halo = lax.ppermute(x_face, "cols", pairs)
        return x_halo, exchange(z_face, "slabs")

    halos = [send(s[4], x_up, s[5]) for s in state]
    low, low_stats = last_half(low_span, *zip(*halos), [0] * chunks, None)
    scaled, end = close(low, starts, low_span, low_stats, field_values.shape, None)
    halos = [send(state[-1][3], x_down, state[-1][6])]
    if chunks > 1:
        halos = [send(state[-1][7], x_down, state[-1][8])] * (chunks - 1) + halos
    high, high_stats = last_half(high_span, *zip(*halos), [*starts[:-1], 0], scaled)
    end = write_parts(high, starts, high_span, end)
    (scaled,) = close(high, starts, high_span, high_stats, field_values.shape, scaled)
    return scaled, end


def solution(mesh):
    spec = P(("site", "rows"), "cols", "slabs", None)

    return jax.shard_map(local, mesh=mesh, in_specs=(spec, spec), out_specs=(spec, spec), check_vma=False)
```

```python
import functools

import jax
import jax.numpy as jnp
from jax import lax
from jax.experimental import pallas as pl
from jax.experimental.pallas import tpu as pltpu
from jax.sharding import PartitionSpec as P


STEPS = 6
CHUNKS = (1, 2, 2, 1)
EPS = 0.0001
VMEM_GRANT = 16 << 20


VMEM_SPEC = pl.BlockSpec(memory_space=pltpu.VMEM)
ANY_SPEC = pl.BlockSpec(memory_space=pl.ANY)
PARAMS = pltpu.CompilerParams(vmem_limit_bytes=VMEM_GRANT)


def in_vmem(value):
    return pltpu.with_memory_space_constraint(value, pltpu.VMEM)


def in_hbm(value):
    return pltpu.with_memory_space_constraint(value, pltpu.HBM)


def vmem_out(*shape):
    return pltpu.VMEM(shape, jnp.float32)


def cost(shape, flops_per_cell, arrays):
    cells = 1
    for size in shape:
        cells *= size
    return pl.CostEstimate(flops=flops_per_cell * cells, bytes_accessed=4 * arrays * cells, transcendentals=0)


def split(length, shares):
    edges = [length * sum(shares[:i]) // sum(shares) for i in range(len(shares) + 1)]
    return [(a, b - a) for a, b in zip(edges[:-1], edges[1:]) if b > a]


def store_faces(row, planes, x_low, x_high, z_faces):
    last_x, last_z = len(planes) - 1, planes[0].shape[0] - 1
    x_low[row] = planes[0]
    x_high[row] = planes[last_x]
    at = 0
    for z_face in z_faces:
        for x in range(z_face.shape[2]):
            z_face[0, row, x:x + 1, :] = planes[at + x][0:1, :]
            z_face[1, row, x:x + 1, :] = planes[at + x][last_z:last_z + 1, :]
        at += z_face.shape[2]


def open_kernel(start, parts, whole, after, field, y_first, y_last, x_face, z_face, sems):
    rows, xs = field.shape[0], field.shape[1]
    copies = [
        pltpu.make_async_copy(whole.at[pl.ds(start + at, size)], field.at[pl.ds(at, size)], sems.at[part])
        for part, (at, size) in enumerate(parts)
    ]
    for copy in copies:
        copy.start()

    def row_faces(row, carry):
        store_faces(row, [field[row, x] for x in range(xs)], x_face.at[0], x_face.at[1], [z_face])
        return carry

    for copy, (at, size) in zip(copies, parts):
        copy.wait()
        lax.fori_loop(at, at + size, row_faces, 0, unroll=4)
    y_first[...] = field[0]
    y_last[...] = field[rows - 1]


def open_chunk(field_values, after, start, rows):
    _, xs, zs, levels = field_values.shape
    parts = split(rows, (1,) * 4)
    outs = [vmem_out(rows, xs, zs, levels), vmem_out(xs, zs, levels), vmem_out(xs, zs, levels)]
    outs += [vmem_out(2, rows, zs, levels), vmem_out(2, rows, xs, levels)]
    return pl.pallas_call(
        functools.partial(open_kernel, start, parts),
        out_shape=tuple(outs),
        in_specs=[ANY_SPEC] * 2,
        out_specs=(VMEM_SPEC,) * len(outs),
        scratch_shapes=[pltpu.SemaphoreType.DMA((len(parts),))],
        compiler_params=PARAMS,
        cost_estimate=cost((rows, xs, zs, levels), 4, 2),
        name="open_chunk",
    )(in_hbm(field_values), after)


def update_rows(start, span, field, crowding, y_before, y_after, x_before, x_after, z_before, z_after,
                out, finish, total):
    rows, xs, zs, levels = field.shape
    x0, x1 = span
    place = lax.broadcasted_iota(jnp.int32, (zs, levels), 0)
    is_first, is_last = place == 0, place == zs - 1

    def planes(ref, row):
        return [ref[row, x] for x in range(x0, x1)]

    def advance(row, below, here, above, total):
        first = x_before[row] if x0 == 0 else field[row, x0 - 1]
        final = x_after[row] if x1 == xs else field[row, x1]
        along = [first, *here, final]
        new = []
        for i, u in enumerate(here):
            near = jnp.broadcast_to(z_before[row, i:i + 1, :], (zs, levels))
            far = jnp.broadcast_to(z_after[row, i:i + 1, :], (zs, levels))
            near = jnp.where(is_first, near, pltpu.roll(u, 1, 0))
            far = jnp.where(is_last, far, pltpu.roll(u, zs - 1, 0))
            around = (along[i] + along[i + 2]) + (near + far) + (below[i] + above[i])
            new.append(0.1 * around + u * (0.6 - 0.2 * (u * crowding[start + row, x0 + i])))
        for i, u in enumerate(new):
            out[row, i] = u
        return finish(row, new, total)

    def body(row, total):
        return advance(row, planes(field, row - 1), planes(field, row), planes(field, row + 1), total)

    top = [y_before[x] for x in range(x0, x1)]
    bottom = [y_after[x] for x in range(x0, x1)]
    total = advance(0, top, planes(field, 0), planes(field, 1), total)
    total = lax.fori_loop(1, rows - 1, body, total, unroll=3 * xs // (x1 - x0))
    return advance(rows - 1, planes(field, rows - 2), planes(field, rows - 1), bottom, total)


def sides(halo):
    return (halo[0].at[1], halo[0].at[0]) if len(halo) == 1 else tuple(halo)


def step_kernel(start, x_count, z_count, halves, gathers, *refs):
    field, crowding, y_before, y_after = refs[:4]
    x_before, x_after = sides(refs[4:4 + x_count])
    z_before, z_after = sides(refs[4 + x_count:4 + x_count + z_count])
    held = refs[5 + x_count + z_count:5 + x_count + z_count + 2 * gathers]
    outs = refs[5 + x_count + z_count + 2 * gathers:]
    out, y_first, y_last = outs[:3]
    if halves:
        x_low, x_high, *z_faces = outs[3:7]
    else:
        x_face, *z_faces = outs[3:]
        x_low, x_high = x_face.at[0], x_face.at[1]

    def finish(row, new, total):
        store_faces(row, new, x_low, x_high, z_faces)
        return total

    update_rows(start, (0, field.shape[1]), field, crowding, y_before, y_after, x_before, x_after,
                z_before, z_after, out, finish, 0)
    y_first[...] = out[0]
    y_last[...] = out[field.shape[0] - 1]
    if gathers:
        x_all, z_all = outs[7:]
        at = 0
        for low, face in zip(held[:gathers], held[gathers:]):
            rows = low.shape[0]
            x_all[at:at + rows] = low[...]
            z_all[:, at:at + rows] = face[...]
            at += rows


def step_chunk(field, crowding, y_before, y_after, x_halo, z_halo, start, after, halves, held):
    rows, xs, zs, levels = field.shape
    gathers = len(held)
    operands = [field, crowding, y_before, y_after, *x_halo, *z_halo, after]
    operands += [low for low, _ in held] + [face for _, face in held]
    outs = [vmem_out(rows, xs, zs, levels), vmem_out(xs, zs, levels), vmem_out(xs, zs, levels)]
    if halves:
        cut = half(xs)
        outs += [vmem_out(rows, zs, levels)] * 2
        outs += [vmem_out(2, rows, cut, levels), vmem_out(2, rows, xs - cut, levels)]
        if gathers:
            before = sum(low.shape[0] for low, _ in held)
            outs += [vmem_out(before, zs, levels), vmem_out(2, before, xs - cut, levels)]
    else:
        outs += [vmem_out(2, rows, zs, levels), vmem_out(2, rows, xs, levels)]
    return pl.pallas_call(
        functools.partial(step_kernel, start, len(x_halo), len(z_halo), halves, gathers),
        out_shape=tuple(outs),
        in_specs=[VMEM_SPEC] * len(operands),
        out_specs=(VMEM_SPEC,) * len(outs),
        compiler_params=PARAMS,
        cost_estimate=cost((rows, xs, zs, levels), 16, 3),
        name="step",
    )(*[in_vmem(operand) for operand in operands])


def half(xs):
    return xs // 2


def merge(groups):
    count, mean, square = groups[0]
    for other_count, other_mean, other_square in groups[1:]:
        both = count + other_count
        apart = other_mean - mean
        mean = mean + apart * (other_count / both)
        square = square + other_square + (apart * apart) * (count * other_count / both)
        count = both
    return count, mean, square


def last_kernel(start, span, halo_at, z_count, earlier, waits, *refs):
    field, crowding, y_before, y_after, x_halo = refs[:5]
    x0, x1 = span
    rows = field.shape[0]
    here = pl.ds(halo_at, rows)
    x_side = x_halo.at[here]
    z_before, z_after = [side.at[here] for side in sides(refs[5:5 + z_count])]
    rest = refs[5 + z_count:]
    earlier_stats = rest[0] if earlier else None
    out, stats = rest[earlier + waits:]

    def finish(row, new, total):
        if total is None:
            return new, [jnp.zeros_like(u) for u in new], [jnp.zeros_like(u) for u in new]
        base, sums, squares = total
        away = [u - b for u, b in zip(new, base)]
        sums = [s + d for s, d in zip(sums, away)]
        squares = [q + d * d for q, d in zip(squares, away)]
        return base, sums, squares

    base, sums, squares = update_rows(
        start, span, field, crowding, y_before, y_after, x_side, x_side, z_before, z_after,
        out, finish, None)
    for i in range(x1 - x0):
        mean = base[i] + sums[i] * (1.0 / rows)
        square = squares[i] - sums[i] * sums[i] * (1.0 / rows)
        groups = [(rows, mean, square)]
        if earlier:
            groups = [(start, earlier_stats[0, i], earlier_stats[1, i])] + groups
        _, stats[0, i], stats[1, i] = merge(groups)


def last_chunk(field, crowding, y_before, y_after, x_halo, z_halo, start, span, halo_at, earlier_stats, wait):
    rows, _, zs, levels = field.shape
    wide = span[1] - span[0]
    operands = [in_vmem(v) for v in (field, crowding, y_before, y_after, x_halo, *z_halo)]
    specs = [VMEM_SPEC] * len(operands)
    if earlier_stats is not None:
        operands.append(in_vmem(earlier_stats))
        specs.append(VMEM_SPEC)
    if wait is not None:
        operands.append(in_hbm(wait))
        specs.append(ANY_SPEC)
    return pl.pallas_call(
        functools.partial(
            last_kernel, start, span, halo_at, len(z_halo), earlier_stats is not None, wait is not None),
        out_shape=(vmem_out(rows, wide, zs, levels), vmem_out(2, wide, zs, levels)),
        in_specs=specs,
        out_specs=(VMEM_SPEC,) * 2,
        compiler_params=PARAMS,
        cost_estimate=cost((rows, wide, zs, levels), 20, 3),
        name="last_step",
    )(*operands)


def part_copies(parts, starts, span, end, sems):
    return [
        pltpu.make_async_copy(
            part, end.at[pl.ds(start, part.shape[0]), pl.ds(span[0], part.shape[1])], sems.at[c])
        for c, (part, start) in enumerate(zip(parts, starts))
    ]


def write_kernel(starts, span, *refs):
    chunks = len(starts)
    end, sems = refs[-2:]
    copies = part_copies(refs[:chunks], starts, span, end, sems)
    for copy in copies:
        copy.start()
    for copy in copies:
        copy.wait()


def write_parts(parts, starts, span, end):
    return pl.pallas_call(
        functools.partial(write_kernel, starts, span),
        out_shape=jax.ShapeDtypeStruct(end.shape, end.dtype),
        in_specs=[VMEM_SPEC] * len(parts) + [ANY_SPEC],
        out_specs=ANY_SPEC,
        input_output_aliases={len(parts): 0},
        scratch_shapes=[pltpu.SemaphoreType.DMA((len(parts),))],
        compiler_params=PARAMS,
        cost_estimate=cost(parts[0].shape, 4 * len(parts), 2),
        name="write_parts",
    )(*[in_vmem(part) for part in parts], end)


def close_kernel(starts, span, others, pieces, first, *refs):
    chunks = len(starts)
    parts = refs[:chunks]
    stats = refs[chunks:chunks + 1 + others]
    copies = []
    if first:
        scaled, end, stage, sems, end_sems = refs[chunks + 1 + others:]
        copies = part_copies(parts, starts, span, end, end_sems)
        for copy in copies:
            copy.start()
    else:
        scaled, stage, sems = refs[chunks + 2 + others:]
    x0, x1 = span
    wide = x1 - x0
    length = stage.shape[0]
    means, gains = [], []
    for i in range(wide):
        count, mean, square = merge([(length, s[0, i], s[1, i]) for s in stats])
        means.append(mean)
        gains.append(lax.rsqrt(square * (1.0 / count) + EPS))
    for piece, (c, at, size) in enumerate(pieces):
        base = starts[c]

        def scale(row, carry, part=parts[c], base=base):
            for i in range(wide):
                stage[base + row, i] = (part[row, i] - means[i]) * gains[i]
            return carry

        lax.fori_loop(at, at + size, scale, 0, unroll=8)
        copy = pltpu.make_async_copy(
            stage.at[pl.ds(base + at, size)], scaled.at[pl.ds(base + at, size), pl.ds(x0, wide)], sems.at[piece])
        copy.start()
        copies.append(copy)
    for copy in copies:
        copy.wait()


def close(parts, starts, span, stats, shape, scaled):
    first = scaled is None
    length, _, zs, levels = shape
    wide = span[1] - span[0]
    whole = jax.ShapeDtypeStruct(shape, jnp.float32)
    pieces = [(c, at, size) for c, f in enumerate(parts) for at, size in split(f.shape[0], (1,) * 2)]
    operands = [in_vmem(v) for v in (*parts, *stats)]
    specs = [VMEM_SPEC] * len(operands)
    if not first:
        operands.append(scaled)
        specs.append(ANY_SPEC)
    outs = (whole, whole) if first else (whole,)
    scratch = [pltpu.VMEM((length, wide, zs, levels), jnp.float32), pltpu.SemaphoreType.DMA((len(pieces),))]
    return pl.pallas_call(
        functools.partial(close_kernel, starts, span, len(stats) - 1, pieces, first),
        out_shape=outs,
        in_specs=specs,
        out_specs=(ANY_SPEC,) * len(outs),
        input_output_aliases={} if first else {len(operands) - 1: 0},
        scratch_shapes=scratch + ([pltpu.SemaphoreType.DMA((len(parts),))] if first else []),
        compiler_params=PARAMS,
        cost_estimate=cost((length, wide, zs, levels), 3, 4),
        name="close",
    )(*operands)


def ring(axis):
    devices = lax.axis_size(axis)
    up = [(i, (i + 1) % devices) for i in range(devices)]
    return devices, up, [(j, i) for i, j in up]


def exchange(face, axis):
    devices, up, down = ring(axis)
    if devices <= 2:
        return (lax.ppermute(face, axis, up),)
    return (lax.ppermute(face[1], axis, up), lax.ppermute(face[0], axis, down))


def local(field_values, crowding):
    length, xs = field_values.shape[:2]
    pieces = split(length, CHUNKS)
    starts = [start for start, _ in pieces]
    chunks = len(pieces)
    devices, up, down = ring("rows")
    _, x_up, x_down = ring("cols")
    state = []
    for start, rows in pieces:
        state.append(open_chunk(field_values, state[-1][1] if state else field_values, start, rows))
    gathered = max(chunks - 2, 0)
    for step in range(STEPS - 1):
        halos = []
        for s in state:
            x_halo = exchange(s[3], "cols")
            halos.append((x_halo, exchange(s[4], "slabs")))
        before = lax.ppermute(state[-1][2], "rows", up)
        after = lax.ppermute(state[0][1], "rows", down)
        new = []
        for c, (s, (x_halo, z_halo), start) in enumerate(zip(state, halos, starts)):
            y_before = before if c == 0 else state[c - 1][2]
            y_after = after if c == chunks - 1 else state[c + 1][1]
            halves = step == STEPS - 2
            held = [(n[3], n[6]) for n in new[:gathered]] if halves and c == chunks - 1 else []
            new.append(step_chunk(s[0], crowding, y_before, y_after, x_halo, z_halo, start,
                                  new[-1][1] if new else s[1], halves, held))
        state = new
    before = lax.ppermute(state[-1][2], "rows", up)
    after = lax.ppermute(state[0][1], "rows", down)
    hops = [[(i, (i + hop) % devices) for i in range(devices)] for hop in range(1, devices)]
    cut = half(xs)
    low_span, high_span = (0, cut), (cut, xs)

    def last_half(span, x_halos, z_halos, offsets, wait):
        parts, stats = [], None
        for c, s in enumerate(state):
            y_before = before if c == 0 else state[c - 1][2]
            y_after = after if c == chunks - 1 else state[c + 1][1]
            part, stats = last_chunk(
                s[0], crowding, y_before, y_after, x_halos[c], z_halos[c], starts[c], span, offsets[c], stats,
                wait if c == chunks - 1 else None)
            parts.append(part)
        return parts, [stats, *[lax.ppermute(stats, "rows", hop) for hop in hops]]

    def send(x_face, pairs, z_face):
        x_halo = lax.ppermute(x_face, "cols", pairs)
        return x_halo, exchange(z_face, "slabs")

    halos = [send(s[4], x_up, s[5]) for s in state]
    low, low_stats = last_half(low_span, *zip(*halos), [0] * chunks, None)
    scaled, end = close(low, starts, low_span, low_stats, field_values.shape, None)
    halos = []
    if gathered:
        halos = [send(state[-1][7], x_down, state[-1][8])] * gathered
    halos += [send(state[c][3], x_down, state[c][6]) for c in range(gathered, chunks)]
    high, high_stats = last_half(high_span, *zip(*halos), [*starts[:gathered], *[0] * (chunks - gathered)], scaled)
    end = write_parts(high, starts, high_span, end)
    (scaled,) = close(high, starts, high_span, high_stats, field_values.shape, scaled)
    return scaled, end


def solution(mesh):
    spec = P(("site", "rows"), "cols", "slabs", None)

    return jax.shard_map(local, mesh=mesh, in_specs=(spec, spec), out_specs=(spec, spec), check_vma=False)
```
